32 devices in a mesh: group: 1, pool: 1, slab: 32 (over z, y, x, core).
Axes of the slice: x: 2, y: 2, z: 4, core: 2. Of those that a mesh axis runs over, the one named last changes fastest.
Arguments:
- drho_part: float32 [1, 16, 2, 128, 128, 128], P('pool', 'group', None, 'slab'), may hold values from -6 to 6
- fxc: float32 [128, 128, 128], P('slab'), may hold values from -2 to -0.2
- cutoff_mask: int32 [128, 128, 128], P(None, 'slab'), may hold values 0 or 1
- owner_table: int32 [16], P('group'), may hold values from 0 to 15, each once
Outputs:
- dv: float32 [16, 2, 128, 128, 128], P('group', None, 'slab')
The draws below stay inside these ranges and needn't reach their ends.
Inputs may be any that keep to these rules, and one draw needn't show every extreme that they name: `owner_table`: each perturbation appears in exactly one slot.
All inputs are finite; a program needn't handle non-finite values. No bound on the sum of `cutoff_mask` on one device may be relied on, other than what follows from the above.
Results may differ from the reference program's by a relative error of at most 0.00008.
Values sent between devices are 32-bit elements; how exact they have to be, the bound alone decides.
A program may use at most 128 MiB of HBM per device.

```python
import math
import jax
import jax.numpy as jnp
from jax import lax

NG = 128
P_SIZE = 16
N_POOL = 1


def set_ends(array, rng, smallest, top_value):
    longest = array.shape.index(max(array.shape))
    spots = []
    for shift in (0, 1):
        where = [jax.random.randint(jax.random.fold_in(rng, axis), (), 0, length) for axis, length in enumerate(array.shape)]
        where[longest] = (where[longest] + shift) % array.shape[longest]
        spots.append(tuple(where))
    return array.at[spots[0]].set(smallest).at[spots[1]].set(top_value)


def shard_levels(stream_key, extent, cuts, low, top_value):
    level, own = 1.0, jax.random.fold_in(stream_key, 6)
    for position, shards_of in cuts:
        steps = jnp.exp(jax.random.uniform(jax.random.fold_in(own, position), (shards_of,), jnp.float32, low / len(cuts), top_value / len(cuts)))
        level = level * jnp.repeat(steps, extent[position] // shards_of).reshape([-1 if axis == position else 1 for axis in range(len(extent))])
    return level


def gaussian(stream_key, extent, width, reach, pieces=(), kind=jnp.bfloat16):
    drawn = jax.random.normal(stream_key, extent, jnp.float32) * width
    if len(pieces) > 0:
        drawn = shard_levels(stream_key, extent, pieces, -0.22, 0.18) * drawn
    return jnp.clip(drawn, min=-reach, max=reach).astype(kind)


def setup_inputs(seed: int = 0, part: int = 0) -> dict:
    key_of = jax.random.split(jax.random.key(seed), 5)
    own_keys = jax.random.split(jax.random.fold_in(key_of[4], part), 5)
    drho_part = gaussian(own_keys[0], (N_POOL, P_SIZE, 2, NG, NG, NG), 1.0, 6.0, ((3, 32),), jnp.float32)
    fxc = jnp.clip(-2.0 + 1.8 * jax.random.uniform(key_of[1], (NG, NG, NG), jnp.float32) ** shard_levels(key_of[1], (NG, NG, NG), ((0, 32),), -0.2, 0.2), -2.0, -0.2)
    cutoff_mask = set_ends((jax.random.randint(key_of[2], (NG, NG, NG), 0, 4) < 3).astype(jnp.int32), jax.random.fold_in(key_of[2], 1), 0, 1)
    owner_table = jax.random.permutation(own_keys[3], P_SIZE).astype(jnp.int32)
    return dict(drho_part=drho_part, fxc=fxc, cutoff_mask=cutoff_mask, owner_table=owner_table)


def kernel_table(cutoff_mask):
    index = jnp.arange(NG, dtype=jnp.int32)
    freq = ((index + NG // 2) % NG - NG // 2).astype(jnp.float32)
    square = freq * freq
    total = square[:, None, None] + square[None, :, None] + square[None, None, :]
    unit = (2.0 * math.pi / NG) ** 2
    return 4.0 * math.pi * cutoff_mask.astype(jnp.float32) / (unit * total + 0.25)


def reference(drho_part, fxc, cutoff_mask, owner_table):
    density = jnp.sum(drho_part, axis=0)
    ordered = jnp.take(density, owner_table, axis=0)
    kernel = kernel_table(cutoff_mask)

    def single(field):
        spectrum = jnp.fft.fftn(lax.complex(field[0], field[1]))
        hartree = jnp.fft.ifftn(spectrum * kernel)
        return jnp.stack([jnp.real(hartree) + fxc * field[0], jnp.imag(hartree) + fxc * field[1]])

    return lax.map(single, ordered)
```

```python
import functools
import math

import jax
import jax.numpy as jnp
import numpy as np
from jax import lax
from jax.experimental import pallas as pl
from jax.experimental.pallas import tpu as pltpu
from jax.sharding import PartitionSpec as P

VMEM_MIB = 50
MESH = pl.DeviceIdType.MESH


def halves(matrix):
    high = matrix.astype(np.float32).astype(jnp.bfloat16)
    low = (matrix - high.astype(np.float64)).astype(np.float32).astype(jnp.bfloat16)
    return np.stack([high, low])


def complex_dft(length, sign):
    index = np.arange(length)
    angle = (index[:, None] * index[None, :] % length) * (2.0 * math.pi / length)
    cosine, sine = np.cos(angle), sign * np.sin(angle)
    return np.block([[cosine, -sine], [sine, cosine]])


def slab_order(length, width):
    table = np.arange(2 * length).reshape(2, length // width, width)
    return table.transpose(1, 0, 2).reshape(-1)


def inner_order(length, width):
    table = np.arange(2 * length).reshape(2, length // width, width)
    return table.transpose(2, 0, 1).reshape(-1)


def split(value):
    high = value.astype(jnp.bfloat16)
    low = (value - high.astype(jnp.float32)).astype(jnp.bfloat16)
    return high, low


def dot(left, right):
    return jnp.dot(left, right, preferred_element_type=jnp.float32)


def left_dot(matrix_ref, value):
    high, low = split(value)
    return dot(matrix_ref[0], high) + (dot(matrix_ref[1], high) + dot(matrix_ref[0], low))


def right_dot(value, matrix_ref):
    high, low = split(value)
    return dot(high, matrix_ref[0]) + (dot(low, matrix_ref[0]) + dot(high, matrix_ref[1]))


def forward_stage(field_ref, along_z_ref, along_y_ref, out_ref):
    _, width, length, _ = field_ref.shape
    slabs = length // width
    rows = width * length
    field = jnp.concatenate([field_ref[c].reshape(rows, length) for c in range(2)], axis=1)
    field = right_dot(field, along_z_ref)
    field = jnp.concatenate(
        [
            jnp.concatenate(
                [field[x * length : (x + 1) * length, c * length : (c + 1) * length] for c in range(2)], axis=0
            )
            for x in range(width)
        ],
        axis=1,
    )
    field = left_dot(along_y_ref, field)
    for y in range(width):
        for c in range(2):
            first = (y * 2 + c) * slabs
            for x in range(width):
                out_ref[:, c * width + x, y * length : (y + 1) * length] = field[
                    first : first + slabs, x * length : (x + 1) * length
                ]


def column_stage(field_ref, screen_ref, forth_ref, back_ref, out_ref):
    slabs, rows, lanes = field_ref.shape
    length = screen_ref.shape[0]
    field = left_dot(forth_ref, field_ref[...].reshape(slabs * rows, lanes))
    screen = screen_ref[...]
    field = jnp.concatenate([field[:length] * screen, field[length:] * screen], axis=0)
    out_ref[...] = left_dot(back_ref, field).reshape(slabs, rows, lanes)


def backward_stage(field_ref, fxc_ref, along_y_ref, along_z_ref, out_ref):
    _, width, length, _ = out_ref.shape
    field = jnp.concatenate(
        [
            jnp.concatenate(
                [field_ref[:, c * width + x, y * length : (y + 1) * length] for y in range(width) for c in range(2)],
                axis=0,
            )
            for x in range(width)
        ],
        axis=1,
    )
    field = left_dot(along_y_ref, field)
    field = jnp.concatenate(
        [
            jnp.concatenate(
                [field[c * length : (c + 1) * length, x * length : (x + 1) * length] for c in range(2)], axis=1
            )
            for x in range(width)
        ],
        axis=0,
    )
    field = right_dot(field, along_z_ref)
    fxc = fxc_ref[...]
    for c in range(2):
        part = field[:, c * length : (c + 1) * length].reshape(width, length, length)
        out_ref[c] = part + fxc * out_ref[c]


def frequency(index, length):
    return (lax.rem(index + length // 2, length) - length // 2).astype(jnp.float32)


def fill_screen(mask_ref, screen_ref, me):
    length, width, _ = mask_ref.shape
    shape = (length, length)
    unit = (2.0 * math.pi / length) ** 2
    along_x = frequency(lax.broadcasted_iota(jnp.int32, shape, 0), length)
    along_z = frequency(lax.broadcasted_iota(jnp.int32, shape, 1), length)
    plane = along_x * along_x + along_z * along_z
    for y in range(width):
        along_y = frequency(jnp.full(shape, me * width + y, jnp.int32), length)
        total = unit * (plane + along_y * along_y) + 0.25
        kept = mask_ref[:, y, :].astype(jnp.float32)
        screen_ref[:, y * length : (y + 1) * length] = 4.0 * math.pi * kept / total * (1.0 / float(length**3))


def exchange_kernel(
    density_ref,
    fxc_hbm,
    mask_hbm,
    z_forth_hbm,
    y_forth_hbm,
    x_forth_hbm,
    x_back_hbm,
    y_back_hbm,
    z_back_hbm,
    result_ref,
    out_forth,
    in_forth,
    out_back,
    in_back,
    screen_ref,
    fxc_ref,
    mask_ref,
    z_forth_ref,
    y_forth_ref,
    x_forth_ref,
    x_back_ref,
    y_back_ref,
    z_back_ref,
    load_sem,
    table_sem,
    out_forth_sem,
    in_forth_sem,
    out_back_sem,
    in_back_sem,
):
    count, slabs, _, _ = out_forth.shape
    me = lax.axis_index("slab")

    def load(p):
        return pltpu.make_async_copy(density_ref.at[p], result_ref.at[p], load_sem.at[p])

    pairs = (
        (z_forth_hbm, z_forth_ref),
        (y_forth_hbm, y_forth_ref),
        (mask_hbm, mask_ref),
        (x_forth_hbm, x_forth_ref),
        (x_back_hbm, x_back_ref),
        (fxc_hbm, fxc_ref),
        (y_back_hbm, y_back_ref),
        (z_back_hbm, z_back_ref),
    )
    tables = [pltpu.make_async_copy(source, target, table_sem.at[k]) for k, (source, target) in enumerate(pairs)]

    def send(source, target, out_sem, in_sem, p):
        def one(step, carry):
            peer = lax.rem(me + step, slabs)
            pltpu.make_async_remote_copy(
                source.at[p, peer],
                target.at[p, me],
                out_sem.at[p],
                in_sem.at[p],
                device_id={"slab": peer},
                device_id_type=MESH,
            ).start()
            return carry

        lax.fori_loop(1, slabs, one, 0)

    def whole(source, target, out_sem, in_sem, p):
        others = pl.ds(0, slabs - 1)
        return pltpu.make_async_remote_copy(
            source.at[p, others],
            target.at[p, others],
            out_sem.at[p],
            in_sem.at[p],
            device_id={"slab": me},
            device_id_type=MESH,
        )

    forth = (out_forth, in_forth, out_forth_sem, in_forth_sem)
    back = (out_back, in_back, out_back_sem, in_back_sem)

    load(0).start()
    for table in tables[:2]:
        table.start()
    barrier = pltpu.get_barrier_semaphore()

    def greet(step, carry):
        pl.semaphore_signal(
            barrier, inc=1, device_id={"slab": lax.rem(me + step, slabs)}, device_id_type=MESH
        )
        return carry

    lax.fori_loop(1, slabs, greet, 0)

    def load_rest(p, carry):
        load(p).start()
        return carry

    lax.fori_loop(1, count, load_rest, 0)
    for table in tables[2:]:
        table.start()

    def forward(p):
        load(p).wait()
        forward_stage(result_ref.at[p], z_forth_ref, y_forth_ref, out_forth.at[p])
        in_forth[p, me] = out_forth[p, me]

    for table in tables[:2]:
        table.wait()
    forward(0)
    pl.semaphore_wait(barrier, slabs - 1)
    send(*forth, 0)

    def forward_step(p, carry):
        forward(p)
        send(*forth, p)
        return carry

    lax.fori_loop(1, count, forward_step, 0)

    for table in tables[2:]:
        table.wait()
    fill_screen(mask_ref, screen_ref, me)

    def column_step(p, carry):
        whole(*forth, p).wait_recv()
        column_stage(in_forth.at[p], screen_ref, x_forth_ref, x_back_ref, out_back.at[p])
        in_back[p, me] = out_back[p, me]
        send(*back, p)
        return carry

    lax.fori_loop(0, count, column_step, 0)

    def backward_step(p, carry):
        whole(*back, p).wait_recv()
        backward_stage(in_back.at[p], fxc_ref, y_back_ref, z_back_ref, result_ref.at[p])
        return carry

    lax.fori_loop(0, count, backward_step, 0)

    def drain(p, carry):
        whole(*forth, p).wait_send()
        whole(*back, p).wait_send()
        return carry

    lax.fori_loop(0, count, drain, 0)


def place_kernel(owner_ref, held_ref, out_ref, sem):
    count = out_ref.shape[0]
    copies = [pltpu.make_async_copy(held_ref.at[owner_ref[slot]], out_ref.at[slot], sem.at[slot]) for slot in range(count)]
    for copy in copies:
        copy.start()
    for copy in copies:
        copy.wait()


def per_device(drho_part, fxc, cutoff_mask, owner_table):
    density = drho_part[0]
    if lax.axis_size("pool") > 1:
        density = lax.psum(density, "pool")
    count, _, width, length, _ = density.shape
    slabs = length // width
    rows, lanes = 2 * width, width * length

    forth, back = complex_dft(length, -1.0), complex_dft(length, 1.0)
    by_slab, by_inner = slab_order(length, width), inner_order(length, width)
    tables = (
        halves(forth.T),
        halves(forth[by_inner]),
        halves(forth[:, by_slab]),
        halves(back[by_slab]),
        halves(back[:, by_inner]),
        halves(back.T),
    )
    tables = [jnp.asarray(table) for table in tables]

    packed = pltpu.VMEM((count, slabs, rows, lanes), jnp.float32)
    held = pl.pallas_call(
        exchange_kernel,
        out_shape=pltpu.VMEM(density.shape, jnp.float32),
        in_specs=[pl.BlockSpec(memory_space=pl.ANY)] * 9,
        out_specs=pl.BlockSpec(memory_space=pltpu.VMEM),
        scratch_shapes=[packed] * 4
        + [
            pltpu.VMEM((length, lanes), jnp.float32),
            pltpu.VMEM(fxc.shape, jnp.float32),
            pltpu.VMEM(cutoff_mask.shape, jnp.int32),
        ]
        + [pltpu.VMEM(table.shape, table.dtype) for table in tables]
        + [pltpu.SemaphoreType.DMA((count,)), pltpu.SemaphoreType.DMA((8,))]
        + [pltpu.SemaphoreType.DMA((count,))] * 4,
        compiler_params=pltpu.CompilerParams(
            collective_id=0, has_side_effects=True, vmem_limit_bytes=VMEM_MIB * 2**20
        ),
        cost_estimate=pl.CostEstimate(
            flops=count * 144 * rows * lanes * length * slabs // 2,
            bytes_accessed=density.size * 8,
            transcendentals=0,
        ),
    )(density, fxc, cutoff_mask, *tables)

    return pl.pallas_call(
        place_kernel,
        out_shape=jax.ShapeDtypeStruct(density.shape, jnp.float32),
        in_specs=[pl.BlockSpec(memory_space=pltpu.SMEM), pl.BlockSpec(memory_space=pltpu.VMEM)],
        out_specs=pl.BlockSpec(memory_space=pl.ANY),
        scratch_shapes=[pltpu.SemaphoreType.DMA((count,))],
        compiler_params=pltpu.CompilerParams(vmem_limit_bytes=2**20),
        cost_estimate=pl.CostEstimate(flops=0, bytes_accessed=density.size * 8, transcendentals=0),
    )(owner_table, held)


def solution(mesh):
    placed = (
        P("pool", "group", None, "slab", None, None),
        P("slab", None, None),
        P(None, "slab", None),
        P("group"),
    )
    return jax.shard_map(
        per_device,
        mesh=mesh,
        in_specs=placed,
        out_specs=P("group", None, "slab", None, None),
        check_vma=False,
    )
```

```python
import functools
import math

import jax
import jax.numpy as jnp
import numpy as np
from jax import lax
from jax.experimental import pallas as pl
from jax.experimental.pallas import tpu as pltpu
from jax.sharding import PartitionSpec as P

VMEM_MIB = 40
PLACE_MIB = 8
EARLY = 2
MESH = pl.DeviceIdType.MESH


def halves(matrix):
    high = matrix.astype(np.float32).astype(jnp.bfloat16)
    low = (matrix - high.astype(np.float64)).astype(np.float32).astype(jnp.bfloat16)
    return np.stack([high, low])


def complex_dft(length, sign):
    index = np.arange(length)
    angle = (index[:, None] * index[None, :] % length) * (2.0 * math.pi / length)
    cosine, sine = np.cos(angle), sign * np.sin(angle)
    return np.block([[cosine, -sine], [sine, cosine]])


def slab_order(length, width):
    table = np.arange(2 * length).reshape(2, length // width, width)
    return table.transpose(1, 0, 2).reshape(-1)


def inner_order(length, width):
    table = np.arange(2 * length).reshape(2, length // width, width)
    return table.transpose(2, 0, 1).reshape(-1)


def split(value):
    high = value.astype(jnp.bfloat16)
    low = (value - high.astype(jnp.float32)).astype(jnp.bfloat16)
    return high, low


def dot(left, right):
    return jnp.dot(left, right, preferred_element_type=jnp.float32)


def left_dot(matrix_ref, value):
    high, low = split(value)
    return dot(matrix_ref[0], high) + (dot(matrix_ref[1], high) + dot(matrix_ref[0], low))


def right_dot(value, matrix_ref):
    high, low = split(value)
    return dot(high, matrix_ref[0]) + (dot(low, matrix_ref[0]) + dot(high, matrix_ref[1]))


def forward_stage(field_ref, along_y_ref, out_ref):
    _, width, length, _ = field_ref.shape
    slabs = length // width
    field = jnp.concatenate(
        [jnp.concatenate([field_ref[c, x] for x in range(width)], axis=1) for c in range(2)], axis=0
    )
    field = left_dot(along_y_ref, field)
    for y in range(width):
        for c in range(2):
            first = (y * 2 + c) * slabs
            for x in range(width):
                out_ref[:, c * width + x, y * length : (y + 1) * length] = field[
                    first : first + slabs, x * length : (x + 1) * length
                ]


def column_stage(field_ref, screen_ref, x_forth_ref, z_forth_ref, z_back_ref, x_back_ref, out_ref):
    slabs, rows, lanes = field_ref.shape
    length = screen_ref.shape[1]
    width = lanes // length
    field = left_dot(x_forth_ref, field_ref[...].reshape(slabs * rows, lanes))
    field = jnp.concatenate(
        [
            jnp.concatenate(
                [field[c * length : (c + 1) * length, y * length : (y + 1) * length] for c in range(2)], axis=1
            )
            for y in range(width)
        ],
        axis=0,
    )
    field = right_dot(field, z_forth_ref)
    screen = screen_ref[...]
    field = jnp.concatenate([field[:, :length] * screen, field[:, length:] * screen], axis=1)
    field = right_dot(field, z_back_ref)
    field = jnp.concatenate(
        [
            jnp.concatenate(
                [field[y * length : (y + 1) * length, c * length : (c + 1) * length] for y in range(width)], axis=1
            )
            for c in range(2)
        ],
        axis=0,
    )
    out_ref[...] = left_dot(x_back_ref, field).reshape(slabs, rows, lanes)


def backward_stage(field_ref, fxc_ref, along_y_ref, density_ref, out_ref):
    _, width, length, _ = out_ref.shape
    field = jnp.concatenate(
        [
            jnp.concatenate(
                [field_ref[:, c * width + x, y * length : (y + 1) * length] for y in range(width) for c in range(2)],
                axis=0,
            )
            for x in range(width)
        ],
        axis=1,
    )
    field = left_dot(along_y_ref, field)
    for c in range(2):
        for x in range(width):
            part = field[c * length : (c + 1) * length, x * length : (x + 1) * length]
            out_ref[c, x] = part + fxc_ref[x] * density_ref[c, x]


def frequency(index, length):
    return (lax.rem(index + length // 2, length) - length // 2).astype(jnp.float32)


def fill_screen(mask_ref, screen_ref, me):
    length, width, _ = mask_ref.shape
    shape = (length, length)
    unit = (2.0 * math.pi / length) ** 2
    along_x = frequency(lax.broadcasted_iota(jnp.int32, shape, 0), length)
    along_z = frequency(lax.broadcasted_iota(jnp.int32, shape, 1), length)
    plane = along_x * along_x + along_z * along_z
    for y in range(width):
        along_y = frequency(jnp.full(shape, me * width + y, jnp.int32), length)
        total = unit * (plane + along_y * along_y) + 0.25
        kept = mask_ref[:, y, :].astype(jnp.float32)
        screen_ref[y * length : (y + 1) * length, :] = 4.0 * math.pi * kept / total * (1.0 / float(length**3))


def peer_steps(slabs):
    if slabs & (slabs - 1):
        return [], list(range(1, slabs))
    half = slabs // 2
    order = [0, 6, 2, 4, 1, 7, 3, 5]
    order = [base + k for base in range(0, half, 8) for k in order if base + k < half]
    steps = [step for k in order for step in (half + k, k) if step]
    inner = 2 ** -(-(slabs.bit_length() - 1) // 2)
    near = [step for step in steps if step < inner or step % inner < 2]
    near.sort(key=lambda step: step < half)
    return near, steps


def exchange_kernel(
    density_ref,
    fxc_hbm,
    mask_hbm,
    y_forth_hbm,
    x_forth_hbm,
    z_forth_hbm,
    z_back_hbm,
    x_back_hbm,
    y_back_hbm,
    result_ref,
    in_back,
    fxc_ref,
    y_back_ref,
    out_forth,
    in_forth,
    out_back,
    screen_ref,
    mask_ref,
    y_forth_ref,
    x_forth_ref,
    z_forth_ref,
    z_back_ref,
    x_back_ref,
    load_sem,
    table_sem,
    out_forth_sem,
    in_forth_sem,
    out_back_sem,
    in_back_sem,
    ready_sem,
):
    count, slabs, _, _ = out_forth.shape
    me = lax.axis_index("slab")
    near, steps = peer_steps(slabs)
    far = [step for step in steps if step not in near]
    early = min(EARLY, count) if near and far else 0

    def peer_of(step):
        return lax.bitwise_xor(me, step) if near else lax.rem(me + step, slabs)

    def load(p):
        return pltpu.make_async_copy(density_ref.at[p], result_ref.at[p], load_sem.at[p])

    pairs = (
        (y_forth_hbm, y_forth_ref),
        (mask_hbm, mask_ref),
        (x_forth_hbm, x_forth_ref),
        (z_forth_hbm, z_forth_ref),
        (z_back_hbm, z_back_ref),
        (x_back_hbm, x_back_ref),
        (fxc_hbm, fxc_ref),
        (y_back_hbm, y_back_ref),
    )
    tables = [pltpu.make_async_copy(source, target, table_sem.at[k]) for k, (source, target) in enumerate(pairs)]

    def signal(semaphore, chosen):
        for step in chosen:
            pl.semaphore_signal(semaphore, inc=1, device_id={"slab": peer_of(step)}, device_id_type=MESH)

    def send(source, target, out_sem, in_sem, p, chosen):
        for step in chosen:
            peer = peer_of(step)
            pltpu.make_async_remote_copy(
                source.at[p, peer],
                target.at[p, me],
                out_sem.at[p],
                in_sem.at[p],
                device_id={"slab": peer},
                device_id_type=MESH,
            ).start()

    def whole(source, target, out_sem, in_sem, p):
        others = pl.ds(0, slabs - 1)
        return pltpu.make_async_remote_copy(
            source.at[p, others],
            target.at[p, others],
            out_sem.at[p],
            in_sem.at[p],
            device_id={"slab": me},
            device_id_type=MESH,
        )

    forth = (out_forth, in_forth, out_forth_sem, in_forth_sem)
    back = (out_back, in_back, out_back_sem, in_back_sem)

    barrier = pltpu.get_barrier_semaphore()
    greeted = near if early else steps
    load(0).start()
    tables[0].start()
    signal(barrier, greeted)

    def load_rest(p, carry):
        load(p).start()
        return carry

    lax.fori_loop(1, count, load_rest, 0)
    for table in tables[1:]:
        table.start()

    def forward(p):
        load(p).wait()
        forward_stage(result_ref.at[p], y_forth_ref, out_forth.at[p])
        in_forth[p, me] = out_forth[p, me]

    tables[0].wait()

    def early_step(p, carry):
        forward(p)

        @pl.when(p == 0)
        def _():
            pl.semaphore_wait(barrier, len(greeted))
            signal(ready_sem, near)

        send(*forth, p, near)
        return carry

    def early_rest(p, carry):
        send(*forth, p, far)
        return carry

    def forward_step(p, carry):
        forward(p)
        if not early:

            @pl.when(p == 0)
            def _():
                pl.semaphore_wait(barrier, len(greeted))

        send(*forth, p, steps)
        return carry

    if early:
        lax.fori_loop(0, early, early_step, 0)
        pl.semaphore_wait(ready_sem, len(near))
        lax.fori_loop(0, early, early_rest, 0)
    lax.fori_loop(early, count, forward_step, 0)

    for table in tables[1:]:
        table.wait()
    fill_screen(mask_ref, screen_ref, me)

    def column_step(p, carry):
        whole(*forth, p).wait_recv()
        column_stage(in_forth.at[p], screen_ref, x_forth_ref, z_forth_ref, z_back_ref, x_back_ref, out_back.at[p])
        in_back[p, me] = out_back[p, me]
        send(*back, p, steps)
        return carry

    lax.fori_loop(0, count, column_step, 0)

    def backward_step(p, carry):
        whole(*back, p).wait_recv()
        backward_stage(in_back.at[p], fxc_ref, y_back_ref, result_ref.at[p], result_ref.at[p])
        return carry

    lax.fori_loop(0, count - 1, backward_step, 0)

    def drain(p, carry):
        whole(*forth, p).wait_send()
        whole(*back, p).wait_send()
        return carry

    lax.fori_loop(0, count, drain, 0)
    whole(*back, count - 1).wait_recv()


def place_kernel(owner_ref, held_ref, in_back, fxc_ref, y_back_ref, out_ref, final_ref, sem):
    count = out_ref.shape[0]
    last = count - 1
    owner = [owner_ref[0, slot] for slot in range(count)]
    for slot in range(count):
        copy = pltpu.make_async_copy(held_ref.at[owner[slot]], out_ref.at[slot], sem.at[slot])
        pl.when(owner[slot] != last)(copy.start)
    backward_stage(in_back.at[last], fxc_ref, y_back_ref, held_ref.at[last], final_ref)
    for slot in range(count):
        copy = pltpu.make_async_copy(final_ref, out_ref.at[slot], sem.at[slot])
        pl.when(owner[slot] == last)(copy.start)
    for slot in range(count):
        pltpu.make_async_copy(final_ref, out_ref.at[slot], sem.at[slot]).wait()


def per_device(drho_part, fxc, cutoff_mask, owner_table):
    density = drho_part[0]
    if lax.axis_size("pool") > 1:
        density = lax.psum(density, "pool")
    count, _, width, length, _ = density.shape
    slabs = length // width
    rows, lanes = 2 * width, width * length

    forth, back = complex_dft(length, -1.0), complex_dft(length, 1.0)
    by_slab, by_inner = slab_order(length, width), inner_order(length, width)
    tables = (
        halves(forth[by_inner]),
        halves(forth[:, by_slab]),
        halves(forth.T),
        halves(back.T),
        halves(back[by_slab]),
        halves(back[:, by_inner]),
    )
    tables = [jnp.asarray(table) for table in tables]

    packed = pltpu.VMEM((count, slabs, rows, lanes), jnp.float32)
    placed = [pltpu.VMEM(table.shape, table.dtype) for table in tables]
    whole_fxc = pltpu.VMEM(fxc.shape, jnp.float32)
    in_vmem = pl.BlockSpec(memory_space=pltpu.VMEM)
    anywhere = pl.BlockSpec(memory_space=pl.ANY)
    work = 48 * rows * lanes * length * slabs // 2
    kept = pl.pallas_call(
        exchange_kernel,
        out_shape=[pltpu.VMEM(density.shape, jnp.float32), packed, whole_fxc, placed[5]],
        in_specs=[anywhere] * 9,
        out_specs=[in_vmem] * 4,
        scratch_shapes=[packed] * 3
        + [pltpu.VMEM((lanes, length), jnp.float32), pltpu.VMEM(cutoff_mask.shape, jnp.int32)]
        + placed[:5]
        + [pltpu.SemaphoreType.DMA((count,)), pltpu.SemaphoreType.DMA((8,))]
        + [pltpu.SemaphoreType.DMA((count,))] * 4
        + [pltpu.SemaphoreType.REGULAR],
        compiler_params=pltpu.CompilerParams(
            collective_id=0, has_side_effects=True, vmem_limit_bytes=VMEM_MIB * 2**20
        ),
        cost_estimate=pl.CostEstimate(flops=3 * count * work, bytes_accessed=density.size * 4, transcendentals=0),
    )(density, fxc, cutoff_mask, *tables)

    return pl.pallas_call(
        place_kernel,
        out_shape=jax.ShapeDtypeStruct(density.shape, jnp.float32),
        in_specs=[in_vmem] * 5,
        out_specs=anywhere,
        scratch_shapes=[pltpu.VMEM(density.shape[1:], jnp.float32), pltpu.SemaphoreType.DMA((count,))],
        compiler_params=pltpu.CompilerParams(vmem_limit_bytes=PLACE_MIB * 2**20),
        cost_estimate=pl.CostEstimate(flops=work, bytes_accessed=density.size * 4, transcendentals=0),
    )(owner_table.reshape(1, count), *kept)


def solution(mesh):
    placed = (
        P("pool", "group", None, "slab", None, None),
        P("slab", None, None),
        P(None, "slab", None),
        P("group"),
    )
    return jax.shard_map(
        per_device,
        mesh=mesh,
        in_specs=placed,
        out_specs=P("group", None, "slab", None, None),
        check_vma=False,
    )
```

```python
import functools
import math

import jax
import jax.numpy as jnp
import numpy as np
from jax import lax
from jax.experimental import pallas as pl
from jax.experimental.pallas import tpu as pltpu
from jax.sharding import PartitionSpec as P

VMEM_MIB = 40
PLACE_MIB = 8
EARLY = 2
MESH = pl.DeviceIdType.MESH


def halves(matrix):
    high = matrix.astype(np.float32).astype(jnp.bfloat16)
    low = (matrix - high.astype(np.float64)).astype(np.float32).astype(jnp.bfloat16)
    return np.stack([high, low])


def complex_dft(length, sign):
    index = np.arange(length)
    angle = (index[:, None] * index[None, :] % length) * (2.0 * math.pi / length)
    cosine, sine = np.cos(angle), sign * np.sin(angle)
    return np.block([[cosine, -sine], [sine, cosine]])


def slab_order(length, width):
    table = np.arange(2 * length).reshape(2, length // width, width)
    return table.transpose(1, 0, 2).reshape(-1)


def inner_order(length, width):
    table = np.arange(2 * length).reshape(2, length // width, width)
    return table.transpose(2, 0, 1).reshape(-1)


def split(value):
    high = value.astype(jnp.bfloat16)
    low = (value - high.astype(jnp.float32)).astype(jnp.bfloat16)
    return high, low


def dot(left, right):
    return jnp.dot(left, right, preferred_element_type=jnp.float32)


def left_dot(matrix_ref, value):
    high, low = split(value)
    return dot(matrix_ref[0], high) + (dot(matrix_ref[1], high) + dot(matrix_ref[0], low))


def right_dot(value, matrix_ref):
    high, low = split(value)
    return dot(high, matrix_ref[0]) + (dot(low, matrix_ref[0]) + dot(high, matrix_ref[1]))


def forward_stage(field_ref, along_y_ref, out_ref):
    _, width, length, _ = field_ref.shape
    slabs = length // width
    field = jnp.concatenate(
        [jnp.concatenate([field_ref[c, x] for x in range(width)], axis=1) for c in range(2)], axis=0
    )
    field = left_dot(along_y_ref, field)
    for y in range(width):
        for c in range(2):
            first = (y * 2 + c) * slabs
            for x in range(width):
                out_ref[:, c * width + x, y * length : (y + 1) * length] = field[
                    first : first + slabs, x * length : (x + 1) * length
                ]


def column_stage(field_ref, screen_ref, x_forth_ref, z_forth_ref, z_back_ref, x_back_ref, out_ref):
    slabs, rows, lanes = field_ref.shape
    length = screen_ref.shape[1]
    width = lanes // length
    field = left_dot(x_forth_ref, field_ref[...].reshape(slabs * rows, lanes))
    field = jnp.concatenate(
        [
            jnp.concatenate(
                [field[c * length : (c + 1) * length, y * length : (y + 1) * length] for c in range(2)], axis=1
            )
            for y in range(width)
        ],
        axis=0,
    )
    field = right_dot(field, z_forth_ref)
    screen = screen_ref[...]
    field = jnp.concatenate([field[:, :length] * screen, field[:, length:] * screen], axis=1)
    field = right_dot(field, z_back_ref)
    field = jnp.concatenate(
        [
            jnp.concatenate(
                [field[y * length : (y + 1) * length, c * length : (c + 1) * length] for y in range(width)], axis=1
            )
            for c in range(2)
        ],
        axis=0,
    )
    out_ref[...] = left_dot(x_back_ref, field).reshape(slabs, rows, lanes)


def backward_stage(field_ref, fxc_ref, along_y_ref, density_ref, out_ref):
    _, width, length, _ = out_ref.shape
    field = jnp.concatenate(
        [
            jnp.concatenate(
                [field_ref[:, c * width + x, y * length : (y + 1) * length] for y in range(width) for c in range(2)],
                axis=0,
            )
            for x in range(width)
        ],
        axis=1,
    )
    field = left_dot(along_y_ref, field)
    for c in range(2):
        for x in range(width):
            part = field[c * length : (c + 1) * length, x * length : (x + 1) * length]
            out_ref[c, x] = part + fxc_ref[x] * density_ref[c, x]


def frequency(index, length):
    return (lax.rem(index + length // 2, length) - length // 2).astype(jnp.float32)


def fill_screen(mask_ref, screen_ref, me):
    length, width, _ = mask_ref.shape
    shape = (length, length)
    unit = (2.0 * math.pi / length) ** 2
    along_x = frequency(lax.broadcasted_iota(jnp.int32, shape, 0), length)
    along_z = frequency(lax.broadcasted_iota(jnp.int32, shape, 1), length)
    plane = along_x * along_x + along_z * along_z
    for y in range(width):
        along_y = frequency(jnp.full(shape, me * width + y, jnp.int32), length)
        total = unit * (plane + along_y * along_y) + 0.25
        kept = mask_ref[:, y, :].astype(jnp.float32)
        screen_ref[y * length : (y + 1) * length, :] = 4.0 * math.pi * kept / total * (1.0 / float(length**3))


def peer_steps(slabs):
    if slabs & (slabs - 1):
        return [], list(range(1, slabs))
    half = slabs // 2
    order = [0, 7, 2, 5, 6, 1, 4, 3]
    order = [base + k for base in range(0, half, 8) for k in order if base + k < half]
    steps = [step for k in order for step in (half + k, k) if step]
    inner = 2 ** -(-(slabs.bit_length() - 1) // 2)
    near = [step for step in steps if step < inner or step % inner < 2]
    near.sort(key=lambda step: step < half)
    return near, steps


def exchange_kernel(
    density_ref,
    fxc_hbm,
    mask_hbm,
    y_forth_hbm,
    x_forth_hbm,
    z_forth_hbm,
    z_back_hbm,
    x_back_hbm,
    y_back_hbm,
    result_ref,
    in_back,
    fxc_ref,
    y_back_ref,
    out_forth,
    in_forth,
    out_back,
    screen_ref,
    mask_ref,
    y_forth_ref,
    x_forth_ref,
    z_forth_ref,
    z_back_ref,
    x_back_ref,
    load_sem,
    table_sem,
    out_forth_sem,
    in_forth_sem,
    out_back_sem,
    in_back_sem,
    ready_sem,
):
    count, slabs, _, _ = out_forth.shape
    me = lax.axis_index("slab")
    near, steps = peer_steps(slabs)
    far = [step for step in steps if step not in near]
    early = min(EARLY, count) if near and far else 0

    half, quarter = slabs // 2, slabs // 4

    def peer_of(step):
        if not near:
            return lax.rem(me + step, slabs)
        if step < half:
            return lax.bitwise_xor(me, step)
        return lax.bitwise_xor(lax.bitwise_xor(me, step), lax.bitwise_and(me, quarter))

    def load(p):
        return pltpu.make_async_copy(density_ref.at[p], result_ref.at[p], load_sem.at[p])

    pairs = (
        (y_forth_hbm, y_forth_ref),
        (mask_hbm, mask_ref),
        (x_forth_hbm, x_forth_ref),
        (z_forth_hbm, z_forth_ref),
        (z_back_hbm, z_back_ref),
        (x_back_hbm, x_back_ref),
        (fxc_hbm, fxc_ref),
        (y_back_hbm, y_back_ref),
    )
    tables = [pltpu.make_async_copy(source, target, table_sem.at[k]) for k, (source, target) in enumerate(pairs)]

    def signal(semaphore, chosen):
        for step in chosen:
            pl.semaphore_signal(semaphore, inc=1, device_id={"slab": peer_of(step)}, device_id_type=MESH)

    def send(source, target, out_sem, in_sem, p, chosen):
        for step in chosen:
            peer = peer_of(step)
            pltpu.make_async_remote_copy(
                source.at[p, peer],
                target.at[p, me],
                out_sem.at[p],
                in_sem.at[p],
                device_id={"slab": peer},
                device_id_type=MESH,
            ).start()

    def whole(source, target, out_sem, in_sem, p):
        others = pl.ds(0, slabs - 1)
        return pltpu.make_async_remote_copy(
            source.at[p, others],
            target.at[p, others],
            out_sem.at[p],
            in_sem.at[p],
            device_id={"slab": me},
            device_id_type=MESH,
        )

    forth = (out_forth, in_forth, out_forth_sem, in_forth_sem)
    back = (out_back, in_back, out_back_sem, in_back_sem)

    barrier = pltpu.get_barrier_semaphore()
    greeted = near if early else steps
    for c in range(2):
        pltpu.make_async_copy(density_ref.at[0, c], result_ref.at[0, c], load_sem.at[0]).start()
        pltpu.make_async_copy(y_forth_hbm.at[c], y_forth_ref.at[c], table_sem.at[0]).start()
    signal(barrier, greeted)

    def load_rest(p, carry):
        load(p).start()
        return carry

    lax.fori_loop(1, count, load_rest, 0)
    for table in tables[1:]:
        table.start()

    def forward(p):
        load(p).wait()
        forward_stage(result_ref.at[p], y_forth_ref, out_forth.at[p])
        in_forth[p, me] = out_forth[p, me]

    tables[0].wait()

    def early_step(p, carry):
        forward(p)

        @pl.when(p == 0)
        def _():
            pl.semaphore_wait(barrier, len(greeted))
            signal(ready_sem, near)

        send(*forth, p, near)
        return carry

    def early_rest(p, carry):
        send(*forth, p, far)
        return carry

    def forward_step(p, carry):
        forward(p)
        if not early:

            @pl.when(p == 0)
            def _():
                pl.semaphore_wait(barrier, len(greeted))

        send(*forth, p, steps)
        return carry

    if early:
        lax.fori_loop(0, early, early_step, 0)
        pl.semaphore_wait(ready_sem, len(near))
        lax.fori_loop(0, early, early_rest, 0)
    lax.fori_loop(early, count, forward_step, 0)

    for table in tables[1:]:
        table.wait()
    fill_screen(mask_ref, screen_ref, me)

    def column_step(p, carry):
        whole(*forth, p).wait_recv()
        column_stage(in_forth.at[p], screen_ref, x_forth_ref, z_forth_ref, z_back_ref, x_back_ref, out_back.at[p])
        in_back[p, me] = out_back[p, me]
        send(*back, p, steps)
        return carry

    lax.fori_loop(0, count, column_step, 0)

    def backward_step(p, carry):
        whole(*back, p).wait_recv()
        backward_stage(in_back.at[p], fxc_ref, y_back_ref, result_ref.at[p], result_ref.at[p])
        return carry

    lax.fori_loop(0, count - 1, backward_step, 0)

    def drain(p, carry):
        whole(*forth, p).wait_send()
        whole(*back, p).wait_send()
        return carry

    lax.fori_loop(0, count, drain, 0)
    whole(*back, count - 1).wait_recv()


def place_kernel(owner_ref, held_ref, in_back, fxc_ref, y_back_ref, out_ref, final_ref, sem):
    count = out_ref.shape[0]
    last = count - 1
    owner = [owner_ref[0, slot] for slot in range(count)]
    for slot in range(count):
        copy = pltpu.make_async_copy(held_ref.at[owner[slot]], out_ref.at[slot], sem.at[slot])
        pl.when(owner[slot] != last)(copy.start)
    backward_stage(in_back.at[last], fxc_ref, y_back_ref, held_ref.at[last], final_ref)
    for slot in range(count):
        copy = pltpu.make_async_copy(final_ref, out_ref.at[slot], sem.at[slot])
        pl.when(owner[slot] == last)(copy.start)
    for slot in range(count):
        pltpu.make_async_copy(final_ref, out_ref.at[slot], sem.at[slot]).wait()


def per_device(drho_part, fxc, cutoff_mask, owner_table):
    density = drho_part[0]
    if lax.axis_size("pool") > 1:
        density = lax.psum(density, "pool")
    count, _, width, length, _ = density.shape
    slabs = length // width
    rows, lanes = 2 * width, width * length

    forth, back = complex_dft(length, -1.0), complex_dft(length, 1.0)
    by_slab, by_inner = slab_order(length, width), inner_order(length, width)
    tables = (
        halves(forth[by_inner]),
        halves(forth[:, by_slab]),
        halves(forth.T),
        halves(back.T),
        halves(back[by_slab]),
        halves(back[:, by_inner]),
    )
    tables = [jnp.asarray(table) for table in tables]

    packed = pltpu.VMEM((count, slabs, rows, lanes), jnp.float32)
    placed = [pltpu.VMEM(table.shape, table.dtype) for table in tables]
    whole_fxc = pltpu.VMEM(fxc.shape, jnp.float32)
    in_vmem = pl.BlockSpec(memory_space=pltpu.VMEM)
    anywhere = pl.BlockSpec(memory_space=pl.ANY)
    work = 48 * rows * lanes * length * slabs // 2
    kept = pl.pallas_call(
        exchange_kernel,
        out_shape=[pltpu.VMEM(density.shape, jnp.float32), packed, whole_fxc, placed[5]],
        in_specs=[anywhere] * 9,
        out_specs=[in_vmem] * 4,
        scratch_shapes=[packed] * 3
        + [pltpu.VMEM((lanes, length), jnp.float32), pltpu.VMEM(cutoff_mask.shape, jnp.int32)]
        + placed[:5]
        + [pltpu.SemaphoreType.DMA((count,)), pltpu.SemaphoreType.DMA((8,))]
        + [pltpu.SemaphoreType.DMA((count,))] * 4
        + [pltpu.SemaphoreType.REGULAR],
        compiler_params=pltpu.CompilerParams(
            collective_id=0, has_side_effects=True, vmem_limit_bytes=VMEM_MIB * 2**20
        ),
        cost_estimate=pl.CostEstimate(flops=3 * count * work, bytes_accessed=density.size * 4, transcendentals=0),
    )(density, fxc, cutoff_mask, *tables)

    return pl.pallas_call(
        place_kernel,
        out_shape=jax.ShapeDtypeStruct(density.shape, jnp.float32),
        in_specs=[in_vmem] * 5,
        out_specs=anywhere,
        scratch_shapes=[pltpu.VMEM(density.shape[1:], jnp.float32), pltpu.SemaphoreType.DMA((count,))],
        compiler_params=pltpu.CompilerParams(vmem_limit_bytes=PLACE_MIB * 2**20),
        cost_estimate=pl.CostEstimate(flops=work, bytes_accessed=density.size * 4, transcendentals=0),
    )(owner_table.reshape(1, count), *kept)


def solution(mesh):
    placed = (
        P("pool", "group", None, "slab", None, None),
        P("slab", None, None),
        P(None, "slab", None),
        P("group"),
    )
    return jax.shard_map(
        per_device,
        mesh=mesh,
        in_specs=placed,
        out_specs=P("group", None, "slab", None, None),
        check_vma=False,
    )
```

```python
import functools
import math

import jax
import jax.numpy as jnp
import numpy as np
from jax import lax
from jax.experimental import pallas as pl
from jax.experimental.pallas import tpu as pltpu
from jax.sharding import PartitionSpec as P

VMEM_MIB = 40
PLACE_MIB = 8
EARLY = 2
MESH = pl.DeviceIdType.MESH


def halves(matrix):
    high = matrix.astype(np.float32).astype(jnp.bfloat16)
    low = (matrix - high.astype(np.float64)).astype(np.float32).astype(jnp.bfloat16)
    return np.stack([high, low])


def complex_dft(length, sign):
    index = np.arange(length)
    angle = (index[:, None] * index[None, :] % length) * (2.0 * math.pi / length)
    cosine, sine = np.cos(angle), sign * np.sin(angle)
    return np.block([[cosine, -sine], [sine, cosine]])


def slab_order(length, width):
    table = np.arange(2 * length).reshape(2, length // width, width)
    return table.transpose(1, 0, 2).reshape(-1)


def inner_order(length, width):
    table = np.arange(2 * length).reshape(2, length // width, width)
    return table.transpose(2, 0, 1).reshape(-1)


def split(value):
    high = value.astype(jnp.bfloat16)
    low = (value - high.astype(jnp.float32)).astype(jnp.bfloat16)
    return high, low


def dot(left, right):
    return jnp.dot(left, right, preferred_element_type=jnp.float32)


def left_dot(matrix_ref, value):
    high, low = split(value)
    return dot(matrix_ref[0], high) + (dot(matrix_ref[1], high) + dot(matrix_ref[0], low))


def right_dot(value, matrix_ref):
    high, low = split(value)
    return dot(high, matrix_ref[0]) + (dot(low, matrix_ref[0]) + dot(high, matrix_ref[1]))


def forward_stage(field_ref, along_y_ref, out_ref, begin=0, end=None):
    _, width, length, _ = field_ref.shape
    slabs = length // width
    end = width if end is None else end
    field = jnp.concatenate(
        [jnp.concatenate([field_ref[c, x] for x in range(width)], axis=1) for c in range(2)], axis=0
    )
    field = left_dot(along_y_ref.at[:, 2 * slabs * begin : 2 * slabs * end], field)
    for y in range(begin, end):
        for c in range(2):
            first = ((y - begin) * 2 + c) * slabs
            for x in range(width):
                out_ref[:, c * width + x, y * length : (y + 1) * length] = field[
                    first : first + slabs, x * length : (x + 1) * length
                ]


def column_stage(field_ref, screen_ref, x_forth_ref, z_forth_ref, z_back_ref, x_back_ref, out_ref):
    slabs, rows, lanes = field_ref.shape
    length = screen_ref.shape[1]
    width = lanes // length
    field = left_dot(x_forth_ref, field_ref[...].reshape(slabs * rows, lanes))
    field = jnp.concatenate(
        [
            jnp.concatenate(
                [field[c * length : (c + 1) * length, y * length : (y + 1) * length] for c in range(2)], axis=1
            )
            for y in range(width)
        ],
        axis=0,
    )
    field = right_dot(field, z_forth_ref)
    screen = screen_ref[...]
    field = jnp.concatenate([field[:, :length] * screen, field[:, length:] * screen], axis=1)
    field = right_dot(field, z_back_ref)
    field = jnp.concatenate(
        [
            jnp.concatenate(
                [field[y * length : (y + 1) * length, c * length : (c + 1) * length] for y in range(width)], axis=1
            )
            for c in range(2)
        ],
        axis=0,
    )
    out_ref[...] = left_dot(x_back_ref, field).reshape(slabs, rows, lanes)


def backward_stage(field_ref, fxc_ref, along_y_ref, density_ref, out_ref):
    _, width, length, _ = out_ref.shape
    field = jnp.concatenate(
        [
            jnp.concatenate(
                [field_ref[:, c * width + x, y * length : (y + 1) * length] for y in range(width) for c in range(2)],
                axis=0,
            )
            for x in range(width)
        ],
        axis=1,
    )
    field = left_dot(along_y_ref, field)
    for c in range(2):
        for x in range(width):
            part = field[c * length : (c + 1) * length, x * length : (x + 1) * length]
            out_ref[c, x] = part + fxc_ref[x] * density_ref[c, x]


def frequency(index, length):
    return (lax.rem(index + length // 2, length) - length // 2).astype(jnp.float32)


def fill_screen(mask_ref, screen_ref, me):
    length, width, _ = mask_ref.shape
    shape = (length, length)
    unit = (2.0 * math.pi / length) ** 2
    along_x = frequency(lax.broadcasted_iota(jnp.int32, shape, 0), length)
    along_z = frequency(lax.broadcasted_iota(jnp.int32, shape, 1), length)
    plane = along_x * along_x + along_z * along_z
    for y in range(width):
        along_y = frequency(jnp.full(shape, me * width + y, jnp.int32), length)
        total = unit * (plane + along_y * along_y) + 0.25
        kept = mask_ref[:, y, :].astype(jnp.float32)
        screen_ref[y * length : (y + 1) * length, :] = 4.0 * math.pi * kept / total * (1.0 / float(length**3))


def peer_steps(slabs):
    if slabs & (slabs - 1):
        return [], list(range(1, slabs))
    half = slabs // 2
    order = [0, 7, 2, 5, 6, 1, 4, 3]
    order = [base + k for base in range(0, half, 8) for k in order if base + k < half]
    steps = [step for k in order for step in (half + k, k) if step]
    inner = 2 ** -(-(slabs.bit_length() - 1) // 2)
    near = [step for step in steps if step < inner or step % inner < 2]
    near.sort(key=lambda step: step < half)
    return near, steps


def exchange_kernel(
    density_ref,
    fxc_hbm,
    mask_hbm,
    y_forth_hbm,
    x_forth_hbm,
    z_forth_hbm,
    z_back_hbm,
    x_back_hbm,
    y_back_hbm,
    result_ref,
    in_back,
    fxc_ref,
    y_back_ref,
    out_forth,
    in_forth,
    out_back,
    screen_ref,
    mask_ref,
    y_forth_ref,
    x_forth_ref,
    z_forth_ref,
    z_back_ref,
    x_back_ref,
    load_sem,
    table_sem,
    out_forth_sem,
    in_forth_sem,
    out_back_sem,
    in_back_sem,
    ready_sem,
):
    count, slabs, _, _ = out_forth.shape
    me = lax.axis_index("slab")
    near, steps = peer_steps(slabs)
    far = [step for step in steps if step not in near]
    early = min(EARLY, count) if near and far else 0

    half, quarter = slabs // 2, slabs // 4

    def peer_of(step):
        if not near:
            return lax.rem(me + step, slabs)
        if step < half:
            return lax.bitwise_xor(me, step)
        return lax.bitwise_xor(lax.bitwise_xor(me, step), lax.bitwise_and(me, quarter))

    def load(p):
        return pltpu.make_async_copy(density_ref.at[p], result_ref.at[p], load_sem.at[p])

    pairs = (
        (y_forth_hbm, y_forth_ref),
        (mask_hbm, mask_ref),
        (x_forth_hbm, x_forth_ref),
        (z_forth_hbm, z_forth_ref),
        (z_back_hbm, z_back_ref),
        (x_back_hbm, x_back_ref),
        (fxc_hbm, fxc_ref),
        (y_back_hbm, y_back_ref),
    )
    tables = [pltpu.make_async_copy(source, target, table_sem.at[k]) for k, (source, target) in enumerate(pairs)]

    def signal(semaphore, chosen):
        for step in chosen:
            pl.semaphore_signal(semaphore, inc=1, device_id={"slab": peer_of(step)}, device_id_type=MESH)

    def send(source, target, out_sem, in_sem, p, chosen, part=slice(None)):
        for step in chosen:
            peer = peer_of(step)
            pltpu.make_async_remote_copy(
                source.at[p, peer, :, part],
                target.at[p, me, :, part],
                out_sem.at[p],
                in_sem.at[p],
                device_id={"slab": peer},
                device_id_type=MESH,
            ).start()

    def whole(source, target, out_sem, in_sem, p):
        others = pl.ds(0, slabs - 1)
        return pltpu.make_async_remote_copy(
            source.at[p, others],
            target.at[p, others],
            out_sem.at[p],
            in_sem.at[p],
            device_id={"slab": me},
            device_id_type=MESH,
        )

    forth = (out_forth, in_forth, out_forth_sem, in_forth_sem)
    back = (out_back, in_back, out_back_sem, in_back_sem)

    barrier = pltpu.get_barrier_semaphore()
    greeted = near if early else steps
    for c in range(2):
        pltpu.make_async_copy(density_ref.at[0, c], result_ref.at[0, c], load_sem.at[0]).start()
        pltpu.make_async_copy(y_forth_hbm.at[c], y_forth_ref.at[c], table_sem.at[0]).start()
    signal(barrier, greeted)

    def load_rest(p, carry):
        load(p).start()
        return carry

    lax.fori_loop(1, count, load_rest, 0)
    for table in tables[1:]:
        table.start()

    def forward(p):
        load(p).wait()
        forward_stage(result_ref.at[p], y_forth_ref, out_forth.at[p])
        in_forth[p, me] = out_forth[p, me]

    tables[0].wait()

    def early_step(p, carry):
        forward(p)
        send(*forth, p, near)
        return carry

    def early_rest(p, carry):
        send(*forth, p, far)
        return carry

    def forward_step(p, carry):
        forward(p)
        if not early:

            @pl.when(p == 0)
            def _():
                pl.semaphore_wait(barrier, len(greeted))

        send(*forth, p, steps)
        return carry

    if early:
        width, length, lanes = density_ref.shape[2], density_ref.shape[3], out_forth.shape[3]
        middle = max(width // 2, 1)
        load(0).wait()
        for begin, end in ((0, middle), (middle, width)):
            if begin < end:
                forward_stage(result_ref.at[0], y_forth_ref, out_forth.at[0], begin, end)
                if begin == 0:
                    pl.semaphore_wait(barrier, len(greeted))
                    signal(ready_sem, near)
                send(*forth, 0, near, slice(begin * length, end * length))
        in_forth[0, me] = out_forth[0, me]
        lax.fori_loop(1, early, early_step, 0)
        pl.semaphore_wait(ready_sem, len(near))
        lax.fori_loop(0, early, early_rest, 0)
    lax.fori_loop(early, count, forward_step, 0)

    for table in tables[1:]:
        table.wait()
    fill_screen(mask_ref, screen_ref, me)

    def column_step(p, carry):
        whole(*forth, p).wait_recv()
        column_stage(in_forth.at[p], screen_ref, x_forth_ref, z_forth_ref, z_back_ref, x_back_ref, out_back.at[p])
        in_back[p, me] = out_back[p, me]
        send(*back, p, steps)
        return carry

    lax.fori_loop(0, count, column_step, 0)

    def backward_step(p, carry):
        whole(*back, p).wait_recv()
        backward_stage(in_back.at[p], fxc_ref, y_back_ref, result_ref.at[p], result_ref.at[p])
        return carry

    lax.fori_loop(0, count - 1, backward_step, 0)

    def drain(p, carry):
        whole(*forth, p).wait_send()
        whole(*back, p).wait_send()
        return carry

    lax.fori_loop(0, count, drain, 0)
    whole(*back, count - 1).wait_recv()


def place_kernel(owner_ref, held_ref, in_back, fxc_ref, y_back_ref, out_ref, final_ref, sem):
    count = out_ref.shape[0]
    last = count - 1
    owner = [owner_ref[0, slot] for slot in range(count)]
    for slot in range(count):
        copy = pltpu.make_async_copy(held_ref.at[owner[slot]], out_ref.at[slot], sem.at[slot])
        pl.when(owner[slot] != last)(copy.start)
    backward_stage(in_back.at[last], fxc_ref, y_back_ref, held_ref.at[last], final_ref)
    for slot in range(count):
        copy = pltpu.make_async_copy(final_ref, out_ref.at[slot], sem.at[slot])
        pl.when(owner[slot] == last)(copy.start)
    for slot in range(count):
        pltpu.make_async_copy(final_ref, out_ref.at[slot], sem.at[slot]).wait()


def per_device(drho_part, fxc, cutoff_mask, owner_table):
    density = drho_part[0]
    if lax.axis_size("pool") > 1:
        density = lax.psum(density, "pool")
    count, _, width, length, _ = density.shape
    slabs = length // width
    rows, lanes = 2 * width, width * length

    forth, back = complex_dft(length, -1.0), complex_dft(length, 1.0)
    by_slab, by_inner = slab_order(length, width), inner_order(length, width)
    tables = (
        halves(forth[by_inner]),
        halves(forth[:, by_slab]),
        halves(forth.T),
        halves(back.T),
        halves(back[by_slab]),
        halves(back[:, by_inner]),
    )
    tables = [jnp.asarray(table) for table in tables]

    packed = pltpu.VMEM((count, slabs, rows, lanes), jnp.float32)
    placed = [pltpu.VMEM(table.shape, table.dtype) for table in tables]
    whole_fxc = pltpu.VMEM(fxc.shape, jnp.float32)
    in_vmem = pl.BlockSpec(memory_space=pltpu.VMEM)
    anywhere = pl.BlockSpec(memory_space=pl.ANY)
    work = 48 * rows * lanes * length * slabs // 2
    kept = pl.pallas_call(
        exchange_kernel,
        out_shape=[pltpu.VMEM(density.shape, jnp.float32), packed, whole_fxc, placed[5]],
        in_specs=[anywhere] * 9,
        out_specs=[in_vmem] * 4,
        scratch_shapes=[packed] * 3
        + [pltpu.VMEM((lanes, length), jnp.float32), pltpu.VMEM(cutoff_mask.shape, jnp.int32)]
        + placed[:5]
        + [pltpu.SemaphoreType.DMA((count,)), pltpu.SemaphoreType.DMA((8,))]
        + [pltpu.SemaphoreType.DMA((count,))] * 4
        + [pltpu.SemaphoreType.REGULAR],
        compiler_params=pltpu.CompilerParams(
            collective_id=0, has_side_effects=True, vmem_limit_bytes=VMEM_MIB * 2**20
        ),
        cost_estimate=pl.CostEstimate(flops=3 * count * work, bytes_accessed=density.size * 4, transcendentals=0),
    )(density, fxc, cutoff_mask, *tables)

    return pl.pallas_call(
        place_kernel,
        out_shape=jax.ShapeDtypeStruct(density.shape, jnp.float32),
        in_specs=[in_vmem] * 5,
        out_specs=anywhere,
        scratch_shapes=[pltpu.VMEM(density.shape[1:], jnp.float32), pltpu.SemaphoreType.DMA((count,))],
        compiler_params=pltpu.CompilerParams(vmem_limit_bytes=PLACE_MIB * 2**20),
        cost_estimate=pl.CostEstimate(flops=work, bytes_accessed=density.size * 4, transcendentals=0),
    )(owner_table.reshape(1, count), *kept)


def solution(mesh):
    placed = (
        P("pool", "group", None, "slab", None, None),
        P("slab", None, None),
        P(None, "slab", None),
        P("group"),
    )
    return jax.shard_map(
        per_device,
        mesh=mesh,
        in_specs=placed,
        out_specs=P("group", None, "slab", None, None),
        check_vma=False,
    )
```

```python
import functools
import math

import jax
import jax.numpy as jnp
import numpy as np
from jax import lax
from jax.experimental import pallas as pl
from jax.experimental.pallas import tpu as pltpu
from jax.sharding import PartitionSpec as P

VMEM_MIB = 40
PLACE_MIB = 8
EARLY = 2
MESH = pl.DeviceIdType.MESH


def halves(matrix):
    high = matrix.astype(np.float32).astype(jnp.bfloat16)
    low = (matrix - high.astype(np.float64)).astype(np.float32).astype(jnp.bfloat16)
    return np.stack([high, low])


def complex_dft(length, sign):
    index = np.arange(length)
    angle = (index[:, None] * index[None, :] % length) * (2.0 * math.pi / length)
    cosine, sine = np.cos(angle), sign * np.sin(angle)
    return np.block([[cosine, -sine], [sine, cosine]])


def slab_order(length, width):
    table = np.arange(2 * length).reshape(2, length // width, width)
    return table.transpose(1, 0, 2).reshape(-1)


def inner_order(length, width):
    table = np.arange(2 * length).reshape(2, length // width, width)
    return table.transpose(2, 0, 1).reshape(-1)


def split(value):
    high = value.astype(jnp.bfloat16)
    low = (value - high.astype(jnp.float32)).astype(jnp.bfloat16)
    return high, low


def dot(left, right):
    return jnp.dot(left, right, preferred_element_type=jnp.float32)


def left_dot(matrix_ref, value):
    high, low = split(value)
    return dot(matrix_ref[0], high) + (dot(matrix_ref[1], high) + dot(matrix_ref[0], low))


def right_dot(value, matrix_ref):
    high, low = split(value)
    return dot(high, matrix_ref[0]) + (dot(low, matrix_ref[0]) + dot(high, matrix_ref[1]))


def forward_stage(field_ref, along_y_ref, out_ref, begin=0, end=None):
    _, width, length, _ = field_ref.shape
    slabs = length // width
    end = width if end is None else end
    field = jnp.concatenate(
        [jnp.concatenate([field_ref[c, x] for x in range(width)], axis=1) for c in range(2)], axis=0
    )
    field = left_dot(along_y_ref.at[:, 2 * slabs * begin : 2 * slabs * end], field)
    for y in range(begin, end):
        for c in range(2):
            first = ((y - begin) * 2 + c) * slabs
            for x in range(width):
                out_ref[:, c * width + x, y * length : (y + 1) * length] = field[
                    first : first + slabs, x * length : (x + 1) * length
                ]


def column_stage(field_ref, screen_ref, x_forth_ref, z_forth_ref, z_back_ref, x_back_ref, out_ref):
    slabs, rows, lanes = field_ref.shape
    length = screen_ref.shape[1]
    width = lanes // length
    field = left_dot(x_forth_ref, field_ref[...].reshape(slabs * rows, lanes))
    field = jnp.concatenate(
        [
            jnp.concatenate(
                [field[c * length : (c + 1) * length, y * length : (y + 1) * length] for c in range(2)], axis=1
            )
            for y in range(width)
        ],
        axis=0,
    )
    field = right_dot(field, z_forth_ref)
    screen = screen_ref[...]
    field = jnp.concatenate([field[:, :length] * screen, field[:, length:] * screen], axis=1)
    field = right_dot(field, z_back_ref)
    field = jnp.concatenate(
        [
            jnp.concatenate(
                [field[y * length : (y + 1) * length, c * length : (c + 1) * length] for y in range(width)], axis=1
            )
            for c in range(2)
        ],
        axis=0,
    )
    out_ref[...] = left_dot(x_back_ref, field).reshape(slabs, rows, lanes)


def backward_stage(field_ref, fxc_ref, along_y_ref, density_ref, out_ref):
    _, width, length, _ = out_ref.shape
    field = jnp.concatenate(
        [
            jnp.concatenate(
                [field_ref[:, c * width + x, y * length : (y + 1) * length] for y in range(width) for c in range(2)],
                axis=0,
            )
            for x in range(width)
        ],
        axis=1,
    )
    field = left_dot(along_y_ref, field)
    for c in range(2):
        for x in range(width):
            part = field[c * length : (c + 1) * length, x * length : (x + 1) * length]
            out_ref[c, x] = part + fxc_ref[x] * density_ref[c, x]


def frequency(index, length):
    return (lax.rem(index + length // 2, length) - length // 2).astype(jnp.float32)


def fill_screen(mask_ref, screen_ref, me):
    length, width, _ = mask_ref.shape
    shape = (length, length)
    unit = (2.0 * math.pi / length) ** 2
    along_x = frequency(lax.broadcasted_iota(jnp.int32, shape, 0), length)
    along_z = frequency(lax.broadcasted_iota(jnp.int32, shape, 1), length)
    plane = along_x * along_x + along_z * along_z
    for y in range(width):
        along_y = frequency(jnp.full(shape, me * width + y, jnp.int32), length)
        total = unit * (plane + along_y * along_y) + 0.25
        kept = mask_ref[:, y, :].astype(jnp.float32)
        screen_ref[y * length : (y + 1) * length, :] = 4.0 * math.pi * kept / total * (1.0 / float(length**3))


def peer_steps(slabs):
    if slabs & (slabs - 1):
        return [], list(range(1, slabs))
    half = slabs // 2
    order = [0, 7, 2, 5, 6, 1, 4, 3]
    order = [base + k for base in range(0, half, 8) for k in order if base + k < half]
    steps = [step for k in order for step in (half + k, k) if step]
    inner = 2 ** -(-(slabs.bit_length() - 1) // 2)
    near = [step for step in steps if step < inner or step % inner < 2]
    near.sort(key=lambda step: step < half)
    return near, steps


def exchange_kernel(
    density_ref,
    fxc_hbm,
    mask_hbm,
    y_forth_hbm,
    x_forth_hbm,
    z_forth_hbm,
    z_back_hbm,
    x_back_hbm,
    y_back_hbm,
    result_ref,
    in_back,
    fxc_ref,
    y_back_ref,
    out_forth,
    in_forth,
    out_back,
    screen_ref,
    mask_ref,
    y_forth_ref,
    x_forth_ref,
    z_forth_ref,
    z_back_ref,
    x_back_ref,
    load_sem,
    table_sem,
    out_forth_sem,
    in_forth_sem,
    out_back_sem,
    in_back_sem,
    ready_sem,
):
    count, slabs, _, _ = out_forth.shape
    me = lax.axis_index("slab")
    near, steps = peer_steps(slabs)
    far = [step for step in steps if step not in near]
    early = min(EARLY, count) if near and far else 0

    half, quarter = slabs // 2, slabs // 4

    def peer_of(step):
        if not near:
            return lax.rem(me + step, slabs)
        if step < half:
            return lax.bitwise_xor(me, step)
        return lax.bitwise_xor(lax.bitwise_xor(me, step), lax.bitwise_and(me, quarter))

    def load(p):
        return pltpu.make_async_copy(density_ref.at[p], result_ref.at[p], load_sem.at[p])

    pairs = (
        (y_forth_hbm, y_forth_ref),
        (mask_hbm, mask_ref),
        (x_forth_hbm, x_forth_ref),
        (z_forth_hbm, z_forth_ref),
        (z_back_hbm, z_back_ref),
        (x_back_hbm, x_back_ref),
        (fxc_hbm, fxc_ref),
        (y_back_hbm, y_back_ref),
    )
    tables = [pltpu.make_async_copy(source, target, table_sem.at[k]) for k, (source, target) in enumerate(pairs)]

    def signal(semaphore, chosen):
        for step in chosen:
            pl.semaphore_signal(semaphore, inc=1, device_id={"slab": peer_of(step)}, device_id_type=MESH)

    def send(source, target, out_sem, in_sem, p, chosen, part=slice(None)):
        for step in chosen:
            peer = peer_of(step)
            pltpu.make_async_remote_copy(
                source.at[p, peer, :, part],
                target.at[p, me, :, part],
                out_sem.at[p],
                in_sem.at[p],
                device_id={"slab": peer},
                device_id_type=MESH,
            ).start()

    def whole(source, target, out_sem, in_sem, p):
        others = pl.ds(0, slabs - 1)
        return pltpu.make_async_remote_copy(
            source.at[p, others],
            target.at[p, others],
            out_sem.at[p],
            in_sem.at[p],
            device_id={"slab": me},
            device_id_type=MESH,
        )

    forth = (out_forth, in_forth, out_forth_sem, in_forth_sem)
    back = (out_back, in_back, out_back_sem, in_back_sem)

    barrier = pltpu.get_barrier_semaphore()
    greeted = near if early else steps
    for c in range(2):
        pltpu.make_async_copy(density_ref.at[0, c], result_ref.at[0, c], load_sem.at[0]).start()
        pltpu.make_async_copy(y_forth_hbm.at[c], y_forth_ref.at[c], table_sem.at[0]).start()
    signal(barrier, greeted)

    def load_rest(p, carry):
        load(p).start()
        return carry

    soon = max(min(early, count), 1)
    lax.fori_loop(1, soon, load_rest, 0)

    def forward(p):
        load(p).wait()
        forward_stage(result_ref.at[p], y_forth_ref, out_forth.at[p])
        in_forth[p, me] = out_forth[p, me]

    def load_later():
        lax.fori_loop(soon, count, load_rest, 0)
        for table in tables[1:]:
            table.start()

    tables[0].wait()

    def early_step(p, carry):
        forward(p)
        send(*forth, p, near)
        return carry

    def early_rest(p, carry):
        send(*forth, p, far)
        return carry

    def forward_step(p, carry):
        forward(p)
        if not early:

            @pl.when(p == 0)
            def _():
                pl.semaphore_wait(barrier, len(greeted))

        send(*forth, p, steps)
        return carry

    if early:
        width, length, lanes = density_ref.shape[2], density_ref.shape[3], out_forth.shape[3]
        middle = max(width // 2, 1)
        load(0).wait()
        load_later()
        for begin, end in ((0, middle), (middle, width)):
            if begin < end:
                forward_stage(result_ref.at[0], y_forth_ref, out_forth.at[0], begin, end)
                if begin == 0:
                    pl.semaphore_wait(barrier, len(greeted))
                    signal(ready_sem, near)
                send(*forth, 0, near, slice(begin * length, end * length))
        in_forth[0, me] = out_forth[0, me]
        lax.fori_loop(1, early, early_step, 0)
        pl.semaphore_wait(ready_sem, len(near))
        lax.fori_loop(0, early, early_rest, 0)
    else:
        load_later()
    lax.fori_loop(early, count, forward_step, 0)

    for table in tables[1:]:
        table.wait()
    fill_screen(mask_ref, screen_ref, me)

    def column_step(p, carry):
        whole(*forth, p).wait_recv()
        column_stage(in_forth.at[p], screen_ref, x_forth_ref, z_forth_ref, z_back_ref, x_back_ref, out_back.at[p])
        in_back[p, me] = out_back[p, me]
        send(*back, p, steps)
        return carry

    lax.fori_loop(0, count, column_step, 0)

    def backward_step(p, carry):
        whole(*back, p).wait_recv()
        backward_stage(in_back.at[p], fxc_ref, y_back_ref, result_ref.at[p], result_ref.at[p])
        return carry

    lax.fori_loop(0, count - 1, backward_step, 0)

    def drain(p, carry):
        whole(*forth, p).wait_send()
        whole(*back, p).wait_send()
        return carry

    lax.fori_loop(0, count, drain, 0)
    whole(*back, count - 1).wait_recv()


def place_kernel(owner_ref, held_ref, in_back, fxc_ref, y_back_ref, out_ref, final_ref, sem):
    count = out_ref.shape[0]
    last = count - 1
    owner = [owner_ref[0, slot] for slot in range(count)]
    for slot in range(count):
        copy = pltpu.make_async_copy(held_ref.at[owner[slot]], out_ref.at[slot], sem.at[slot])
        pl.when(owner[slot] != last)(copy.start)
    backward_stage(in_back.at[last], fxc_ref, y_back_ref, held_ref.at[last], final_ref)
    for slot in range(count):
        copy = pltpu.make_async_copy(final_ref, out_ref.at[slot], sem.at[slot])
        pl.when(owner[slot] == last)(copy.start)
    for slot in range(count):
        pltpu.make_async_copy(final_ref, out_ref.at[slot], sem.at[slot]).wait()


def per_device(drho_part, fxc, cutoff_mask, owner_table):
    density = drho_part[0]
    if lax.axis_size("pool") > 1:
        density = lax.psum(density, "pool")
    count, _, width, length, _ = density.shape
    slabs = length // width
    rows, lanes = 2 * width, width * length

    forth, back = complex_dft(length, -1.0), complex_dft(length, 1.0)
    by_slab, by_inner = slab_order(length, width), inner_order(length, width)
    tables = (
        halves(forth[by_inner]),
        halves(forth[:, by_slab]),
        halves(forth.T),
        halves(back.T),
        halves(back[by_slab]),
        halves(back[:, by_inner]),
    )
    tables = [jnp.asarray(table) for table in tables]

    packed = pltpu.VMEM((count, slabs, rows, lanes), jnp.float32)
    placed = [pltpu.VMEM(table.shape, table.dtype) for table in tables]
    whole_fxc = pltpu.VMEM(fxc.shape, jnp.float32)
    in_vmem = pl.BlockSpec(memory_space=pltpu.VMEM)
    anywhere = pl.BlockSpec(memory_space=pl.ANY)
    work = 48 * rows * lanes * length * slabs // 2
    kept = pl.pallas_call(
        exchange_kernel,
        out_shape=[pltpu.VMEM(density.shape, jnp.float32), packed, whole_fxc, placed[5]],
        in_specs=[anywhere] * 9,
        out_specs=[in_vmem] * 4,
        scratch_shapes=[packed] * 3
        + [pltpu.VMEM((lanes, length), jnp.float32), pltpu.VMEM(cutoff_mask.shape, jnp.int32)]
        + placed[:5]
        + [pltpu.SemaphoreType.DMA((count,)), pltpu.SemaphoreType.DMA((8,))]
        + [pltpu.SemaphoreType.DMA((count,))] * 4
        + [pltpu.SemaphoreType.REGULAR],
        compiler_params=pltpu.CompilerParams(
            collective_id=0, has_side_effects=True, vmem_limit_bytes=VMEM_MIB * 2**20
        ),
        cost_estimate=pl.CostEstimate(flops=3 * count * work, bytes_accessed=density.size * 4, transcendentals=0),
    )(density, fxc, cutoff_mask, *tables)

    return pl.pallas_call(
        place_kernel,
        out_shape=jax.ShapeDtypeStruct(density.shape, jnp.float32),
        in_specs=[in_vmem] * 5,
        out_specs=anywhere,
        scratch_shapes=[pltpu.VMEM(density.shape[1:], jnp.float32), pltpu.SemaphoreType.DMA((count,))],
        compiler_params=pltpu.CompilerParams(vmem_limit_bytes=PLACE_MIB * 2**20),
        cost_estimate=pl.CostEstimate(flops=work, bytes_accessed=density.size * 4, transcendentals=0),
    )(owner_table.reshape(1, count), *kept)


def solution(mesh):
    placed = (
        P("pool", "group", None, "slab", None, None),
        P("slab", None, None),
        P(None, "slab", None),
        P("group"),
    )
    return jax.shard_map(
        per_device,
        mesh=mesh,
        in_specs=placed,
        out_specs=P("group", None, "slab", None, None),
        check_vma=False,
    )
```
